128 devices in a mesh: section: 8 (over z, core), rows: 16 (over y, x).
Axes of the slice: x: 4, y: 4, z: 4, core: 2. Of those that a mesh axis runs over, the one named last changes fastest.
Arguments:
- features: bfloat16 [2048, 1536], P('rows'), may hold values from -6 to 6
- ages: int32 [2048], P('rows'), may hold values from 0 to 15
- age_table: bfloat16 [16, 1536], replicated, may hold values from -3 to 3
- returns: float32 [2048], P('rows'), may hold values from -6 to 6
- owners: int32 [2048, 1], P('rows'), may hold values from 0 to 15; in each aligned block of 128 rows (0 to 127, 128 to 255, ...) at most 32 rows name the same one
- slots: int32 [2048], P('rows'), may hold values from 0 to 4095
- norm_gain: float32 [8, 1536], P('section'), may hold values from 0.1 to 1.9
- w_gate: bfloat16 [8, 1536, 8960], P('section', None, 'rows'), may hold values from -0.15625 to 0.15625
- w_up: bfloat16 [8, 1536, 8960], P('section', None, 'rows'), may hold values from -0.15625 to 0.15625
- w_down: bfloat16 [8, 8960, 1536], P('section', 'rows'), may hold values from -0.0625 to 0.0625
- final_gain: float32 [1536], replicated, may hold values from 0.1 to 1.9
- reward_head: float32 [1536], replicated, may hold values from -0.15625 to 0.15625
- old_priority: float32 [65536], P('rows'), may hold values from 0.05 to 2
Outputs:
- rewards: float32 [2048], P(('rows', 'section'))
- weights: float32 [65536], P(('rows', 'section'))
The draws below stay inside these ranges and needn't reach their ends.
Inputs may be any that keep to these rules, and one draw needn't show every extreme that they name: `owners`: among the rows of one device at most 32 name the same owner; in every draw some owner is named by exactly 32 rows of some device.
All inputs are finite; a program needn't handle non-finite values.
Results may differ from the reference program's by a relative error of at most 0.04.
Values may be sent and summed in bfloat16 or wider, within the bound.
No kernel may reach another device: no remote copies, remote signals or barrier semaphores. Data moves between devices by JAX's collectives and lax.ppermute only.
A program may use at most 64 MiB of HBM per device.

```python
import math
import jax
import jax.numpy as jnp
import numpy as np
from jax import lax

D = 1536
FF = 8960
AGES = 16
CAP = 32
ROWS_DEV = 128
BUF_DEV = 4096
LAYERS = 8
ROWS = 2048
OWNERS = 16
BUF = 65536


def set_ends(result, own_key, low, high):
    longest = result.shape.index(max(result.shape))
    spots = []
    for shift in (0, 1):
        where = [jax.random.randint(jax.random.fold_in(own_key, axis), (), 0, length) for axis, length in enumerate(result.shape)]
        where[longest] = (where[longest] + shift) % result.shape[longest]
        spots.append(tuple(where))
    return result.at[spots[0]].set(low).at[spots[1]].set(high)


def shard_levels(key, extent, cuts, least, high):
    loudness, own = 1.0, jax.random.fold_in(key, 6)
    for axis_at, parts in cuts:
        steps = jnp.exp(jax.random.uniform(jax.random.fold_in(own, axis_at), (parts,), jnp.float32, least / len(cuts), high / len(cuts)))
        loudness = loudness * jnp.repeat(steps, extent[axis_at] // parts).reshape([-1 if axis == axis_at else 1 for axis in range(len(extent))])
    return loudness


def assign_block(stream_key, own, number, rows, amount, top, reach, slope):
    order = jax.random.permutation(stream_key, amount)
    packed, usual = portions_of(amount, rows * top, reach, slope, True), portions_of(amount, rows * top, reach, slope, False)
    places = jnp.arange(amount)

    def named(lengths, rotation):
        used = int((lengths > 0).sum())
        fixed = max(1, used // 4)
        passed = fixed + (places - fixed + rotation * (used - fixed)) % max(1, amount - fixed)
        return jnp.zeros((amount,), jnp.int32).at[order[jnp.where(places < fixed, places, passed)]].set(jnp.asarray(lengths, jnp.int32))

    lengths = jnp.where(number % 4 == 0, named(packed, number // 4), named(usual, number - number // 4 - 1))
    mixed = jax.random.permutation(jax.random.fold_in(own, 3), amount)
    giver, sink = mixed[0:amount // 2 * 2:2], mixed[1:amount // 2 * 2:2]
    margin = jnp.minimum(lengths[giver] - 1, reach - lengths[sink]) // 2
    margin = jnp.where((giver == order[0]) | (sink == order[0]) | (lengths[sink] == 0), 0, jnp.maximum(margin, 0))
    passed = jax.random.randint(jax.random.fold_in(own, 4), (amount // 2,), 0, 1 << 20) % (margin + 1)
    lengths = lengths.at[giver].add(-passed).at[sink].add(passed)
    items = jnp.searchsorted(jnp.cumsum(lengths), jnp.arange(rows * top), side="right").astype(jnp.int32)
    grid = items.reshape(top, rows).T
    grid = grid[jax.random.permutation(jax.random.fold_in(own, 1), rows)]
    rotation = jax.random.randint(jax.random.fold_in(own, 2), (rows, 1), 0, top)
    return jnp.take_along_axis(grid, (jnp.arange(top)[None, :] + rotation) % top, axis=1)


def portions_of(count, total, reach, skew, full):
    loads = [(1 << 20) // math.isqrt(grade ** skew) + 1 for grade in range(1, count + 1)]
    largest = reach if full else min(reach, max(-(-total // count), total * loads[0] // sum(loads)))
    least = 1 if total - largest >= count - 1 else 0
    counts, surplus = [largest] + [least] * (count - 1), total - largest - least * (count - 1)
    while surplus > 0:
        candidates = [i for i in range(1, count) if counts[i] < largest] or [i for i in range(1, count) if counts[i] < reach]
        whole, budget = sum([loads[i] for i in candidates]), surplus
        for i in candidates:
            more = min(reach - counts[i], max(1, budget * loads[i] // whole), surplus)
            counts[i] = counts[i] + more
            surplus = surplus - more
    return np.array(counts)


def normal_values(key, dims, scale, most, split=(), dtype=jnp.bfloat16):
    result = scale * jax.random.normal(key, dims, jnp.float32)
    if split:
        result = result * shard_levels(key, dims, split, -0.22, 0.18)
    return jnp.clip(result, -most, most).astype(dtype)


def setup_inputs(seed: int = 0) -> dict:
    arg_keys = jax.random.split(jax.random.key(seed), 14)
    features = normal_values(arg_keys[0], (ROWS, D), 1.0, 6.0, ((0, 16),))
    ages = set_ends(jax.random.randint(arg_keys[1], (ROWS,), 0, AGES), jax.random.fold_in(arg_keys[1], 1), 0, AGES - 1).astype(jnp.int32)
    age_table = normal_values(arg_keys[2], (AGES, D), 0.5, 3.0)
    returns = normal_values(arg_keys[3], (ROWS,), 1.0, 6.0, ((0, 16),), jnp.float32)
    owners_keys = jax.random.split(jax.random.fold_in(arg_keys[4], 1), ROWS // ROWS_DEV)
    owners_turns = jax.random.permutation(jax.random.fold_in(arg_keys[4], 3), ROWS // ROWS_DEV)
    owners = jax.vmap(lambda own, number: assign_block(jax.random.fold_in(arg_keys[4], 2), own, number, ROWS_DEV, OWNERS, 1, CAP, 2))(owners_keys, owners_turns).reshape((ROWS, 1))
    slots = set_ends(jax.random.randint(arg_keys[5], (ROWS,), 0, BUF_DEV), jax.random.fold_in(arg_keys[5], 1), 0, BUF_DEV - 1).astype(jnp.int32)
    norm_gain = jnp.clip(1.0 + 0.18 * jax.random.normal(arg_keys[6], (LAYERS, D), jnp.float32), 0.1, 1.9)
    w_gate = normal_values(arg_keys[7], (LAYERS, D, FF), D ** -0.5, 0.15625, ((0, 8), (2, 16)))
    w_up = normal_values(arg_keys[8], (LAYERS, D, FF), D ** -0.5, 0.15625, ((0, 8), (2, 16)))
    w_down = normal_values(arg_keys[9], (LAYERS, FF, D), FF ** -0.5, 0.0625, ((0, 8), (1, 16)))
    final_gain = jnp.clip(1.0 + 0.18 * jax.random.normal(arg_keys[10], (D,), jnp.float32), 0.1, 1.9)
    reward_head = normal_values(arg_keys[11], (D,), D ** -0.5, 0.15625, (), jnp.float32)
    old_priority = jnp.clip(jnp.exp(math.log(2.0) - 3.6888794 * jax.random.uniform(arg_keys[12], (BUF,), jnp.float32) ** shard_levels(arg_keys[12], (BUF,), ((0, 16),), -0.2, 0.2)), 0.05, 2.0)
    return dict(features=features, ages=ages, age_table=age_table, returns=returns, owners=owners, slots=slots, norm_gain=norm_gain, w_gate=w_gate, w_up=w_up, w_down=w_down, final_gain=final_gain, reward_head=reward_head, old_priority=old_priority)


def scaled_norm(values, gain):
    return values * lax.rsqrt(lax.optimization_barrier(jnp.mean(values * values, axis=-1, keepdims=True)) + 1e-06) * gain

def reference(features, ages, age_table, returns, owners, slots, norm_gain, w_gate, w_up, w_down, final_gain, reward_head, old_priority):
    onehot = (ages[:, None] == jnp.arange(AGES)[None, :]).astype(jnp.bfloat16)
    state = (features.astype(jnp.float32) + jnp.dot(onehot, age_table, preferred_element_type=jnp.float32)).astype(jnp.bfloat16)
    for layer in range(LAYERS):
        wide = state.astype(jnp.float32)
        normed = scaled_norm(wide, norm_gain[layer]).astype(jnp.bfloat16)
        gate = jnp.dot(normed, w_gate[layer], preferred_element_type=jnp.float32)
        upper = jnp.dot(normed, w_up[layer], preferred_element_type=jnp.float32)
        hidden = (jax.nn.silu(gate) * upper).astype(jnp.bfloat16)
        state = (wide + jnp.dot(hidden, w_down[layer], preferred_element_type=jnp.float32)).astype(jnp.bfloat16)
    finished = scaled_norm(state.astype(jnp.float32), final_gain)
    rewards = lax.optimization_barrier(jnp.sum(finished * reward_head, axis=-1))
    priority = jnp.exp(0.6 * jnp.log(jnp.abs(rewards - returns) + 0.05))
    target = (owners[:, 0] * BUF_DEV + slots).astype(jnp.int32)
    largest = jax.ops.segment_max(priority, target, num_segments=BUF)
    counted = jax.ops.segment_sum(jnp.ones_like(priority), target, num_segments=BUF)
    refreshed = jnp.where(counted > 0, largest, old_priority)
    weights = refreshed * (BUF / jnp.sum(refreshed))
    return (rewards, weights)
```

```python
import functools

import jax
import jax.numpy as jnp
from jax import lax
from jax.experimental import pallas as pl
from jax.experimental.pallas import tpu as pltpu
from jax.sharding import PartitionSpec as P

MICRO = 4
STAGES = 8
BOTH = ("section", "rows")


def place(x, y, z, c):
    return ((z % 4) * 2 + c) * 16 + (y % 4) * 4 + x % 4


CHIPS = [(x, y, z, c) for z in range(4) for c in range(2) for y in range(4) for x in range(4)]


def member(z, p, q, c, y):
    return place(p + 2 * q - 2 * y, y, z, c)


MEMBERS = [(z, p, q, c, y) for z in range(4) for p in range(2) for q in range(2) for c in range(2) for y in range(4)]
FIRST = [
    (place(x, y, z, c), place(x, y - 1, z, c) if c == x % 2 else place(x + 1, y, z, 1 - c)) for x, y, z, c in CHIPS
]
SECOND = [
    (place(x, y, z, c), place(x, y, z, c) if c == x % 2 else place(x - 1, y, z, 1 - c)) for x, y, z, c in CHIPS
]
TWIN = [(place(x, y, z, c), place(x, y, z, 1 - c)) for x, y, z, c in CHIPS]
ENTER = [(place(x - c, y, 3, c), place(x, y, 3, c)) for x in (1, 3) for y in range(4) for c in range(2)]


def onward(d):
    return [(member(z, p, q, c, y), member(z + p, 1 - p, q, c, y + d)) for z, p, q, c, y in MEMBERS]


def back(d):
    return [(member(z, p, q, c, y), member(z, p, q, c, y - d)) for z, p, q, c, y in MEMBERS]


def layer_kernel(*refs):
    rows_in, gain = refs[:4], refs[4]
    gates, ups, downs = refs[5:9], refs[9:13], refs[13:17]
    outs = refs[17:21]
    gate_buf, up_buf, down_buf, normed, total, sems = refs[21:]
    for j in range(4):
        pltpu.make_async_copy(gates[j], gate_buf.at[j], sems.at[0, j]).start()
        pltpu.make_async_copy(ups[j], up_buf.at[j], sems.at[1, j]).start()
        pltpu.make_async_copy(downs[j], down_buf.at[j], sems.at[2, j]).start()
    block = rows_in[0].shape[0]
    for d in range(4):
        wide = rows_in[d][...].astype(jnp.float32)
        scale = lax.rsqrt(jnp.mean(wide * wide, axis=-1, keepdims=True) + 1e-6)
        normed[pl.ds(d * block, block), :] = (wide * scale * gain[...]).astype(jnp.bfloat16)
    total[...] = jnp.zeros_like(total)

    def part(j, carry):
        pltpu.make_async_copy(gates[0], gate_buf.at[j], sems.at[0, j]).wait()
        pltpu.make_async_copy(ups[0], up_buf.at[j], sems.at[1, j]).wait()
        rows = normed[...]
        gate = jnp.dot(rows, gate_buf[j], preferred_element_type=jnp.float32)
        upper = jnp.dot(rows, up_buf[j], preferred_element_type=jnp.float32)
        hidden = (gate / (1.0 + jnp.exp(-gate)) * upper).astype(jnp.bfloat16)
        pltpu.make_async_copy(downs[0], down_buf.at[j], sems.at[2, j]).wait()
        total[...] += jnp.dot(hidden, down_buf[j], preferred_element_type=jnp.float32)
        return carry

    lax.fori_loop(0, 4, part, 0)
    for d in range(4):
        outs[d][...] = total[pl.ds(d * block, block), :].astype(jnp.bfloat16)


def layer_call(blocks, gain, gates, ups, downs):
    block, width = blocks[0].shape
    units = gates[0].shape[1]
    near = pl.BlockSpec(memory_space=pltpu.VMEM)
    far = pl.BlockSpec(memory_space=pl.ANY)
    return pl.pallas_call(
        layer_kernel,
        out_shape=[jax.ShapeDtypeStruct((block, width), jnp.bfloat16)] * 4,
        in_specs=[near] * 5 + [far] * 12,
        out_specs=[near] * 4,
        scratch_shapes=[
            pltpu.VMEM((4, width, units), jnp.bfloat16),
            pltpu.VMEM((4, width, units), jnp.bfloat16),
            pltpu.VMEM((4, units, width), jnp.bfloat16),
            pltpu.VMEM((4 * block, width), jnp.bfloat16),
            pltpu.VMEM((4 * block, width), jnp.float32),
            pltpu.SemaphoreType.DMA((3, 4)),
        ],
        compiler_params=pltpu.CompilerParams(vmem_limit_bytes=40 << 20),
        cost_estimate=pl.CostEstimate(
            flops=2 * 3 * 4 * units * width * 4 * block,
            bytes_accessed=3 * 4 * units * width * 2,
            transcendentals=4 * block * 4 * units,
        ),
    )(*blocks, gain, *gates, *ups, *downs)


def on_device(
    features,
    ages,
    age_table,
    returns,
    owners,
    slots,
    norm_gain,
    w_gate,
    w_up,
    w_down,
    final_gain,
    reward_head,
    old_priority,
):
    section = lax.axis_index("section")
    row_group = lax.axis_index("rows")
    parity = row_group % 2
    native = section % 2 == parity
    last = jnp.logical_and(section >= STAGES - 2, parity == 1)
    rows_here, width = features.shape
    table_size = old_priority.shape[0]
    block = rows_here // MICRO

    def send(value, pairs):
        return lax.ppermute(value, BOTH, pairs)

    entry_rows = send(features, ENTER)
    entry_ages = send(ages, ENTER)
    weights = []
    for shard in (w_gate[0], w_up[0], w_down[0]):
        first, second = send(shard, FIRST), send(shard, SECOND)
        weights.append([first, second, send(first, TWIN), send(second, TWIN)])
    gates, ups, downs = weights
    gain = jnp.where(native, norm_gain, send(norm_gain, TWIN))

    target = (owners[:, 0] * table_size + slots).astype(jnp.float32)
    known = lax.all_gather(jnp.stack([returns, target]), "rows")
    returns_all = known[:, 0].reshape(-1)
    target_all = known[:, 1].reshape(-1)
    count = target_all.shape[0]
    entries = (row_group * table_size + jnp.arange(table_size)).astype(jnp.float32)
    named = jnp.any(target_all[:, None] == entries[None, :], axis=0)
    kept_sum = jnp.sum(jnp.where(named, 0.0, old_priority))
    order = jnp.arange(count)
    repeat = jnp.any(
        jnp.logical_and(target_all[:, None] == target_all[None, :], order[:, None] < order[None, :]), axis=0
    )

    onehot = (entry_ages[:, None] == jnp.arange(age_table.shape[0])[None, :]).astype(jnp.bfloat16)
    entry = (
        entry_rows.astype(jnp.float32) + jnp.dot(onehot, age_table, preferred_element_type=jnp.float32)
    ).astype(jnp.bfloat16)

    state = entry[:block]
    finished = []
    for tick in range(MICRO + STAGES - 1):
        blocks = [send(state, onward(d)) for d in range(4)]
        parts = layer_call(blocks, gain, gates, ups, downs)
        arrived = [send(parts[d], back(d)) for d in range(1, 4)]
        summed = blocks[0].astype(jnp.float32) + parts[0].astype(jnp.float32)
        for piece in arrived:
            summed = summed + piece.astype(jnp.float32)
        state = summed.astype(jnp.bfloat16)
        if tick >= STAGES - 1:
            wide = state.astype(jnp.float32)
            scaled = wide * lax.rsqrt(jnp.mean(wide * wide, axis=-1, keepdims=True) + 1e-6) * final_gain
            finished.append(jnp.sum(scaled * reward_head, axis=-1))
        if tick + 1 < MICRO:
            state = jnp.where(last, entry[(tick + 1) * block : (tick + 2) * block], state)

    mine = jnp.stack([jnp.concatenate(finished), jnp.broadcast_to(kept_sum, (rows_here,))])
    everything = lax.all_gather(mine, BOTH)
    ends = everything[:, 0].reshape(4, 2, 4, 2, 2, rows_here)[3, :, :, :, 1]
    rewards = jnp.flip(ends, 0).transpose(1, 2, 0, 3).reshape(-1)
    kept_total = jnp.sum(everything[:16, 1, 0])
    priority = jnp.exp(0.6 * jnp.log(jnp.abs(rewards - returns_all) + 0.05))
    group_best = jnp.max(jnp.where(target_all[:, None] == target_all[None, :], priority[:, None], 0.0), axis=0)
    total = kept_total + jnp.sum(jnp.where(repeat, 0.0, group_best))
    part = table_size // STAGES
    own_entries = (row_group * table_size + section * part + jnp.arange(part)).astype(jnp.float32)
    best = jnp.max(jnp.where(target_all[:, None] == own_entries[None, :], priority[:, None], 0.0), axis=0)
    own_old = lax.dynamic_slice_in_dim(old_priority, section * part, part, 0)
    refreshed = jnp.where(best > 0.0, best, own_old)
    weights_out = refreshed * (table_size * 16 / total)
    share = rows_here // STAGES
    rewards_out = lax.dynamic_slice_in_dim(rewards, row_group * rows_here + section * share, share, 0)
    return rewards_out, weights_out


def solution(mesh):
    placed = (
        P("rows", None),
        P("rows"),
        P(),
        P("rows"),
        P("rows", None),
        P("rows"),
        P("section", None),
        P("section", None, "rows"),
        P("section", None, "rows"),
        P("section", "rows", None),
        P(),
        P(),
        P("rows"),
    )
    return jax.shard_map(
        on_device,
        mesh=mesh,
        in_specs=placed,
        out_specs=(P(("rows", "section")), P(("rows", "section"))),
        check_vma=False,
    )
```

```python
import functools

import jax
import jax.numpy as jnp
from jax import lax
from jax.experimental import pallas as pl
from jax.experimental.pallas import tpu as pltpu
from jax.sharding import PartitionSpec as P

MICRO = 4
STAGES = 8
BOTH = ("section", "rows")


def place(x, y, z, c):
    return ((z % 4) * 2 + c) * 16 + (y % 4) * 4 + x % 4


def across(at):
    return (at + 1 if at % 2 else at - 1) % 4


def parity_of(x, z):
    return (x // 2) ^ (z % 2)


CHIPS = [(x, y, z, c) for z in range(4) for c in range(2) for y in range(4) for x in range(4)]
FIRST = [
    (place(x, y, z, c), place(x, across(y), z, c) if c == parity_of(x, z) else place(across(x), y, z, 1 - c))
    for x, y, z, c in CHIPS
]
SECOND = [(place(x, y, z, c), place(x, across(y), z, c)) for x, y, z, c in CHIPS if c != parity_of(x, z)]
FROM_HOME = [(place(x, y, z, c), place(x, y, z, 1 - c)) for x, y, z, c in CHIPS if c == parity_of(x, z)]
TO_HOME = [(place(x, y, z, c), place(x, y, z, 1 - c)) for x, y, z, c in CHIPS if c != parity_of(x, z)]
TWIN = [(place(x, y, z, c), place(x, y, z, 1 - c)) for x, y, z, c in CHIPS]
ENTER = [(place(across(x), y, 3, 0), place(x, y, 3, 1)) for x in (0, 1) for y in range(4)]


def onward(d, stages=range(8)):
    pairs = []
    for x, y, z, c in CHIPS:
        parity = parity_of(x, z)
        if 2 * z + parity in stages:
            there = x if parity else across(x)
            pairs.append((place(x, y, z, c), place(there ^ (d & 1), y ^ (d >> 1), z + parity, c)))
    return pairs


def back(d):
    return [(place(x, y, z, c), place(x ^ (d & 1), y ^ (d >> 1), z, c)) for x, y, z, c in CHIPS]


LANES = 128


def pack_kernel(gate, up, out):
    units, width = gate.shape
    whole = units // LANES * LANES
    rest = units - whole
    for at in range(0, whole, LANES):
        out[:, at : at + LANES] = gate[at : at + LANES, :].T
        out[:, whole + at : whole + at + LANES] = up[at : at + LANES, :].T
    filler = jnp.zeros((LANES - 2 * rest, width), gate.dtype)
    ends = jnp.concatenate([gate[whole:, :], up[whole:, :], filler], axis=0)
    out[:, 2 * whole : 2 * whole + LANES] = ends.T


def packed(gate, up):
    units, width = gate.shape
    near = pl.BlockSpec(memory_space=pltpu.VMEM)
    return pl.pallas_call(
        pack_kernel,
        out_shape=jax.ShapeDtypeStruct((width, 2 * (units // LANES * LANES) + LANES), gate.dtype),
        in_specs=[near, near],
        out_specs=near,
        compiler_params=pltpu.CompilerParams(vmem_limit_bytes=32 << 20),
        cost_estimate=pl.CostEstimate(flops=units * width * 400, bytes_accessed=8 * units * width, transcendentals=0),
    )(gate, up)


def gated(gate, upper):
    return (gate / (1.0 + jnp.exp(-gate)) * upper).astype(jnp.bfloat16)


def layer_kernel(*refs):
    native, rows_in, gain = refs[0], refs[1:5], refs[5]
    shards = (refs[6:12], refs[12:18])
    outs = refs[18:22]
    enter_buf, down_buf, normed, total, sems = refs[22:]
    buffers = (enter_buf, down_buf)
    at_home = native[0] == 1

    def fetch(j, kind, source):
        pltpu.make_async_copy(shards[kind][source], buffers[kind].at[j], sems.at[kind, j]).start()

    def drain(j, kind):
        pltpu.make_async_copy(shards[kind][0], buffers[kind].at[j], sems.at[kind, j]).wait()

    for j, (home, away) in enumerate(((0, 2), (1, 1), (5, 3), (4, 4))):
        for kind in range(2):
            if home == away:
                fetch(j, kind, home)
            else:

                @pl.when(at_home)
                def _():
                    fetch(j, kind, home)

                @pl.when(jnp.logical_not(at_home))
                def _():
                    fetch(j, kind, away)

    block = rows_in[0].shape[0]
    for d in range(4):
        wide = rows_in[d][...].astype(jnp.float32)
        scale = lax.rsqrt(jnp.mean(wide * wide, axis=-1, keepdims=True) + 1e-6)
        normed[pl.ds(d * block, block), :] = (wide * scale * gain[...]).astype(jnp.bfloat16)
    total[...] = jnp.zeros_like(total)
    units = down_buf.shape[1]
    whole = units // LANES * LANES
    rest = units - whole

    def part(j, carry):
        drain(j, 0)
        both = jnp.dot(normed[...], enter_buf[j], preferred_element_type=jnp.float32)
        hidden = gated(both[:, :whole], both[:, whole : 2 * whole])
        ends = gated(both[:, 2 * whole : 2 * whole + rest], both[:, 2 * whole + rest : 2 * whole + 2 * rest])
        drain(j, 1)
        total[...] += jnp.dot(hidden, down_buf[j, :whole, :], preferred_element_type=jnp.float32) + jnp.dot(
            ends, down_buf[j, whole:, :], preferred_element_type=jnp.float32
        )
        return carry

    lax.fori_loop(0, 4, part, 0)
    for d in range(4):
        outs[d][...] = total[pl.ds(d * block, block), :].astype(jnp.bfloat16)


def layer_call(native, blocks, gain, enters, downs):
    block, width = blocks[0].shape
    units = downs[0].shape[0]
    near = pl.BlockSpec(memory_space=pltpu.VMEM)
    far = pl.BlockSpec(memory_space=pl.ANY)
    return pl.pallas_call(
        layer_kernel,
        out_shape=[jax.ShapeDtypeStruct((block, width), jnp.bfloat16)] * 4,
        in_specs=[pl.BlockSpec(memory_space=pltpu.SMEM)] + [near] * 5 + [far] * 12,
        out_specs=[near] * 4,
        scratch_shapes=[
            pltpu.VMEM((4, *enters[0].shape), jnp.bfloat16),
            pltpu.VMEM((4, *downs[0].shape), jnp.bfloat16),
            pltpu.VMEM((4 * block, width), jnp.bfloat16),
            pltpu.VMEM((4 * block, width), jnp.float32),
            pltpu.SemaphoreType.DMA((2, 4)),
        ],
        compiler_params=pltpu.CompilerParams(vmem_limit_bytes=56 << 20),
        cost_estimate=pl.CostEstimate(
            flops=2 * 3 * 4 * units * width * 4 * block,
            bytes_accessed=3 * 4 * units * width * 2,
            transcendentals=4 * block * 4 * units,
        ),
    )(native, *blocks, gain, *enters, *downs)


def from_everyone(value, axis):
    copies = jnp.broadcast_to(value, (lax.axis_size(axis), *value.shape))
    return lax.all_to_all(copies, axis, 0, 0, tiled=True)


def on_device(
    features,
    ages,
    age_table,
    returns,
    owners,
    slots,
    norm_gain,
    w_gate,
    w_up,
    w_down,
    final_gain,
    reward_head,
    old_priority,
):
    section = lax.axis_index("section")
    row_group = lax.axis_index("rows")
    half = row_group % 4 // 2
    native = section % 2 == half ^ (section // 2 % 2)
    last = jnp.logical_and(section >= STAGES - 2, half == 0)
    rows_here, width = features.shape
    table_size = old_priority.shape[0]
    block = rows_here // MICRO

    def send(value, pairs):
        return lax.ppermute(value, BOTH, pairs)

    entry_rows = send(features, ENTER)
    entry_ages = send(ages, ENTER)
    enter = packed(w_gate[0].T, w_up[0].T)
    enter_first = send(enter, FIRST)
    target = (owners[:, 0] * table_size + slots).astype(jnp.float32)
    facts, enter = lax.optimization_barrier((jnp.stack([returns, target]), enter))
    known = from_everyone(facts, "rows")
    at_home = section % 2 == 0
    onehot = (jnp.where(at_home, ages, entry_ages)[:, None] == jnp.arange(age_table.shape[0])[None, :]).astype(
        jnp.bfloat16
    )
    entry = (
        jnp.where(at_home, features, entry_rows).astype(jnp.float32)
        + jnp.dot(onehot, age_table, preferred_element_type=jnp.float32)
    ).astype(jnp.bfloat16)
    gain = jnp.where(native, norm_gain, send(norm_gain, TWIN))
    native_flag = native.astype(jnp.int32)[None]
    entry, down, known, enter_first = lax.optimization_barrier((entry, w_down[0], known, enter_first))
    enter_second = send(enter_first, SECOND)
    blocks = [send(entry[:block], onward(d, (STAGES - 1,))) for d in range(4)]
    down_first = send(down, FIRST)

    returns_all = known[:, 0].reshape(-1)
    target_all = known[:, 1].reshape(-1)
    count = target_all.shape[0]
    entries = (row_group * table_size + jnp.arange(table_size)).astype(jnp.float32)
    named = jnp.any(target_all[:, None] == entries[None, :], axis=0)
    kept_sum = jnp.sum(jnp.where(named, 0.0, old_priority))
    order = jnp.arange(count)
    repeat = jnp.any(
        jnp.logical_and(target_all[:, None] == target_all[None, :], order[:, None] < order[None, :]), axis=0
    ).astype(jnp.float32)
    down_first, blocks, kept_sum, repeat, gain = lax.optimization_barrier(
        (down_first, blocks, kept_sum, repeat, gain)
    )
    down_second = send(down_first, SECOND)

    def six(own, first, second):
        return [own, first, second, send(own, FROM_HOME), send(first, TWIN), send(second, TO_HOME)]

    enters, downs = six(enter, enter_first, enter_second), six(down, down_first, down_second)

    def step(blocks):
        parts = layer_call(native_flag, blocks, gain, enters, downs)
        summed = blocks[0].astype(jnp.float32) + parts[0].astype(jnp.float32)
        for piece in [send(parts[d], back(d)) for d in range(1, 4)]:
            summed = summed + piece.astype(jnp.float32)
        return summed.astype(jnp.bfloat16)

    def sent(state):
        return [send(state, onward(d)) for d in range(4)]

    def rewarded(state):
        wide = state.astype(jnp.float32)
        scaled = wide * lax.rsqrt(jnp.mean(wide * wide, axis=-1, keepdims=True) + 1e-6) * final_gain
        return jnp.sum(scaled * reward_head, axis=-1)

    for number in range(1, MICRO):
        blocks = sent(jnp.where(last, entry[number * block : (number + 1) * block], step(blocks)))
    blocks, unused = lax.scan(lambda held, unused: (sent(step(held)), None), blocks, None, length=STAGES - MICRO)
    states = []
    for number in range(MICRO):
        states.append(step(blocks))
        if number + 1 < MICRO:
            blocks = sent(states[-1])
    rewards_here = jnp.concatenate([rewarded(state) for state in states])

    mine = jnp.stack([rewards_here, jnp.broadcast_to(kept_sum, (rows_here,))])
    everything = from_everyone(mine, BOTH).reshape(4, 2, 4, 4, 2, rows_here)[3].transpose(1, 2, 0, 3, 4)
    ends = everything[:, :, :, 0]
    rewards = jnp.stack([ends[:, 0, 0], ends[:, 1, 0], ends[:, 1, 1], ends[:, 0, 1]], axis=1).reshape(-1)
    kept_total = jnp.sum(everything[:, :, 0, 1, 0])
    priority = jnp.exp(0.6 * jnp.log(jnp.abs(rewards - returns_all) + 0.05))
    group_best = jnp.max(jnp.where(target_all[:, None] == target_all[None, :], priority[:, None], 0.0), axis=0)
    total = kept_total + jnp.sum(jnp.where(repeat > 0.0, 0.0, group_best))
    part = table_size // STAGES
    own_entries = (row_group * table_size + section * part + jnp.arange(part)).astype(jnp.float32)
    best = jnp.max(jnp.where(target_all[:, None] == own_entries[None, :], priority[:, None], 0.0), axis=0)
    own_old = lax.dynamic_slice_in_dim(old_priority, section * part, part, 0)
    refreshed = jnp.where(best > 0.0, best, own_old)
    weights_out = refreshed * (table_size * 16 / total)
    share = rows_here // STAGES
    rewards_out = lax.dynamic_slice_in_dim(rewards, row_group * rows_here + section * share, share, 0)
    return rewards_out, weights_out


def solution(mesh):
    placed = (
        P("rows", None),
        P("rows"),
        P(),
        P("rows"),
        P("rows", None),
        P("rows"),
        P("section", None),
        P("section", None, "rows"),
        P("section", None, "rows"),
        P("section", "rows", None),
        P(),
        P(),
        P("rows"),
    )
    return jax.shard_map(
        on_device,
        mesh=mesh,
        in_specs=placed,
        out_specs=(P(("rows", "section")), P(("rows", "section"))),
        check_vma=False,
    )
```

```python
import functools

import jax
import jax.numpy as jnp
from jax import lax
from jax.experimental import pallas as pl
from jax.experimental.pallas import tpu as pltpu
from jax.sharding import PartitionSpec as P

MICRO = 4
STAGES = 8
BOTH = ("section", "rows")


def place(x, y, z, c):
    return ((z % 4) * 2 + c) * 16 + (y % 4) * 4 + x % 4


def across(at):
    return (at + 1 if at % 2 else at - 1) % 4


def parity_of(x, z):
    return (x // 2) ^ (z % 2)


CHIPS = [(x, y, z, c) for z in range(4) for c in range(2) for y in range(4) for x in range(4)]
FIRST = [
    (place(x, y, z, c), place(x, across(y), z, c) if c == parity_of(x, z) else place(across(x), y, z, 1 - c))
    for x, y, z, c in CHIPS
]
SECOND = [(place(x, y, z, c), place(x, across(y), z, c)) for x, y, z, c in CHIPS if c != parity_of(x, z)]
FROM_HOME = [(place(x, y, z, c), place(x, y, z, 1 - c)) for x, y, z, c in CHIPS if c == parity_of(x, z)]
TO_HOME = [(place(x, y, z, c), place(x, y, z, 1 - c)) for x, y, z, c in CHIPS if c != parity_of(x, z)]
TWIN = [(place(x, y, z, c), place(x, y, z, 1 - c)) for x, y, z, c in CHIPS]
ENTER = [(place(across(x), y, 3, 0), place(x, y, 3, 1)) for x in (0, 1) for y in range(4)]


def onward(d, stages=range(8)):
    pairs = []
    for x, y, z, c in CHIPS:
        parity = parity_of(x, z)
        if 2 * z + parity in stages:
            there = x if parity else across(x)
            pairs.append((place(x, y, z, c), place(there ^ (d & 1), y ^ (d >> 1), z + parity, c)))
    return pairs


def back(d):
    return [(place(x, y, z, c), place(x ^ (d & 1), y ^ (d >> 1), z, c)) for x, y, z, c in CHIPS]


LANES = 128
LIMIT = 8 << 20


def pack_kernel(gate, up, out):
    units, width = gate.shape
    whole = units // LANES * LANES
    rest = units - whole
    for at in range(0, whole, LANES):
        out[:, at : at + LANES] = gate[at : at + LANES, :].T
        out[:, whole + at : whole + at + LANES] = up[at : at + LANES, :].T
    filler = jnp.zeros((LANES - 2 * rest, width), gate.dtype)
    ends = jnp.concatenate([gate[whole:, :], up[whole:, :], filler], axis=0)
    out[:, 2 * whole : 2 * whole + LANES] = ends.T


def packed(gate, up):
    units, width = gate.shape
    near = pl.BlockSpec(memory_space=pltpu.VMEM)
    return pl.pallas_call(
        pack_kernel,
        out_shape=jax.ShapeDtypeStruct((width, 2 * (units // LANES * LANES) + LANES), gate.dtype),
        in_specs=[near, near],
        out_specs=near,
        compiler_params=pltpu.CompilerParams(vmem_limit_bytes=32 << 20),
        cost_estimate=pl.CostEstimate(flops=units * width * 400, bytes_accessed=8 * units * width, transcendentals=0),
    )(gate, up)


def gated(gate, upper):
    return (gate / (1.0 + jnp.exp(-gate)) * upper).astype(jnp.bfloat16)


def normalise(rows_in, gain, normed):
    block = rows_in[0].shape[0]
    for d in range(4):
        wide = rows_in[d][...].astype(jnp.float32)
        scale = lax.rsqrt(jnp.mean(wide * wide, axis=-1, keepdims=True) + 1e-6)
        normed[pl.ds(d * block, block), :] = (wide * scale * gain[...]).astype(jnp.bfloat16)


def project(ready, enter_buf, down_buf, outs, normed, total):
    units = down_buf.shape[1]
    whole = units // LANES * LANES
    rest = units - whole
    total[...] = jnp.zeros_like(total)

    def part(j, carry):
        ready(j, 0)
        both = jnp.dot(normed[...], enter_buf[j], preferred_element_type=jnp.float32)
        hidden = gated(both[:, :whole], both[:, whole : 2 * whole])
        ends = gated(both[:, 2 * whole : 2 * whole + rest], both[:, 2 * whole + rest : 2 * whole + 2 * rest])
        ready(j, 1)
        total[...] += jnp.dot(hidden, down_buf[j, :whole, :], preferred_element_type=jnp.float32) + jnp.dot(
            ends, down_buf[j, whole:, :], preferred_element_type=jnp.float32
        )
        return carry

    lax.fori_loop(0, 4, part, 0)
    block = outs[0].shape[0]
    for d in range(4):
        outs[d][...] = total[pl.ds(d * block, block), :].astype(jnp.bfloat16)


def first_kernel(*refs):
    native, rows_in, gain = refs[0], refs[1:5], refs[5]
    shards = (refs[6:12], refs[12:18])
    outs, buffers = refs[18:22], refs[22:24]
    normed, total, sems = refs[24:]
    at_home = native[0] == 1

    def fetch(j, kind, source):
        pltpu.make_async_copy(shards[kind][source], buffers[kind].at[j], sems.at[kind, j]).start()

    def drain(j, kind):
        pltpu.make_async_copy(shards[kind][0], buffers[kind].at[j], sems.at[kind, j]).wait()

    for j, (home, away) in enumerate(((0, 2), (1, 1), (5, 3), (4, 4))):
        for kind in range(2):
            if home == away:
                fetch(j, kind, home)
            else:

                @pl.when(at_home)
                def _():
                    fetch(j, kind, home)

                @pl.when(jnp.logical_not(at_home))
                def _():
                    fetch(j, kind, away)

    normalise(rows_in, gain, normed)
    project(drain, *buffers, outs, normed, total)


def layer_kernel(*refs):
    normed, total = refs[11:]
    normalise(refs[:4], refs[4], normed)
    project(lambda j, kind: None, refs[5], refs[6], refs[7:11], normed, total)


def parts_of(block, width):
    return [jax.ShapeDtypeStruct((block, width), jnp.bfloat16)] * 4


def scratch_of(block, width):
    return [pltpu.VMEM((4 * block, width), jnp.bfloat16), pltpu.VMEM((4 * block, width), jnp.float32)]


def cost_of(block, width, units):
    return pl.CostEstimate(
        flops=2 * 3 * 4 * units * width * 4 * block,
        bytes_accessed=4 * 4 * block * width,
        transcendentals=4 * block * 4 * units,
    )


def first_call(native, blocks, gain, enters, downs):
    block, width = blocks[0].shape
    near = pl.BlockSpec(memory_space=pltpu.VMEM)
    far = pl.BlockSpec(memory_space=pl.ANY)
    enters, downs = ([pltpu.with_memory_space_constraint(w, pltpu.HBM) for w in held] for held in (enters, downs))
    return pl.pallas_call(
        first_kernel,
        out_shape=parts_of(block, width)
        + [pltpu.VMEM((4, *held.shape), jnp.bfloat16) for held in (enters[0], downs[0])],
        in_specs=[pl.BlockSpec(memory_space=pltpu.SMEM)] + [near] * 5 + [far] * 12,
        out_specs=[near] * 6,
        scratch_shapes=scratch_of(block, width) + [pltpu.SemaphoreType.DMA((2, 4))],
        compiler_params=pltpu.CompilerParams(vmem_limit_bytes=LIMIT),
        cost_estimate=cost_of(block, width, downs[0].shape[0]),
    )(native, *blocks, gain, *enters, *downs)


def layer_call(blocks, gain, enters, downs):
    block, width = blocks[0].shape
    near = pl.BlockSpec(memory_space=pltpu.VMEM)
    enters, downs = (pltpu.with_memory_space_constraint(held, pltpu.VMEM) for held in (enters, downs))
    return pl.pallas_call(
        layer_kernel,
        out_shape=parts_of(block, width),
        in_specs=[near] * 7,
        out_specs=[near] * 4,
        scratch_shapes=scratch_of(block, width),
        compiler_params=pltpu.CompilerParams(vmem_limit_bytes=LIMIT),
        cost_estimate=cost_of(block, width, downs.shape[1]),
    )(*blocks, gain, enters, downs)


def from_everyone(value, axis):
    copies = jnp.broadcast_to(value, (lax.axis_size(axis), *value.shape))
    return lax.all_to_all(copies, axis, 0, 0, tiled=True)


def on_device(
    features,
    ages,
    age_table,
    returns,
    owners,
    slots,
    norm_gain,
    w_gate,
    w_up,
    w_down,
    final_gain,
    reward_head,
    old_priority,
):
    section = lax.axis_index("section")
    row_group = lax.axis_index("rows")
    half = row_group % 4 // 2
    native = section % 2 == half ^ (section // 2 % 2)
    last = jnp.logical_and(section >= STAGES - 2, half == 0)
    rows_here, width = features.shape
    table_size = old_priority.shape[0]
    block = rows_here // MICRO

    def send(value, pairs):
        return lax.ppermute(value, BOTH, pairs)

    entry_rows = send(features, ENTER)
    entry_ages = send(ages, ENTER)
    enter = packed(w_gate[0].T, w_up[0].T)
    enter_first = send(enter, FIRST)
    target = (owners[:, 0] * table_size + slots).astype(jnp.float32)
    facts, enter = lax.optimization_barrier((jnp.stack([returns, target]), enter))
    known = from_everyone(facts, "rows")
    at_home = section % 2 == 0
    onehot = (jnp.where(at_home, ages, entry_ages)[:, None] == jnp.arange(age_table.shape[0])[None, :]).astype(
        jnp.bfloat16
    )
    entry = (
        jnp.where(at_home, features, entry_rows).astype(jnp.float32)
        + jnp.dot(onehot, age_table, preferred_element_type=jnp.float32)
    ).astype(jnp.bfloat16)
    gain = jnp.where(native, norm_gain, send(norm_gain, TWIN))
    native_flag = native.astype(jnp.int32)[None]
    entry, down, known, enter_first = lax.optimization_barrier((entry, w_down[0], known, enter_first))
    enter_second = send(enter_first, SECOND)
    blocks = [send(entry[:block], onward(d, (STAGES - 1,))) for d in range(4)]
    down_first = send(down, FIRST)

    returns_all = known[:, 0].reshape(-1)
    target_all = known[:, 1].reshape(-1)
    count = target_all.shape[0]
    entries = (row_group * table_size + jnp.arange(table_size)).astype(jnp.float32)
    named = jnp.any(target_all[:, None] == entries[None, :], axis=0)
    kept_sum = jnp.sum(jnp.where(named, 0.0, old_priority))
    order = jnp.arange(count)
    repeat = jnp.any(
        jnp.logical_and(target_all[:, None] == target_all[None, :], order[:, None] < order[None, :]), axis=0
    ).astype(jnp.float32)
    down_first, blocks, kept_sum, repeat, gain = lax.optimization_barrier(
        (down_first, blocks, kept_sum, repeat, gain)
    )
    down_second = send(down_first, SECOND)

    def six(own, first, second):
        return [own, first, second, send(own, FROM_HOME), send(first, TWIN), send(second, TO_HOME)]

    enters, downs = six(enter, enter_first, enter_second), six(down, down_first, down_second)

    def onto(blocks, parts):
        summed = blocks[0].astype(jnp.float32) + parts[0].astype(jnp.float32)
        for piece in [send(parts[d], back(d)) for d in range(1, 4)]:
            summed = summed + piece.astype(jnp.float32)
        return summed.astype(jnp.bfloat16)

    def sent(state):
        return [send(state, onward(d)) for d in range(4)]

    def rewarded(state):
        wide = state.astype(jnp.float32)
        scaled = wide * lax.rsqrt(jnp.mean(wide * wide, axis=-1, keepdims=True) + 1e-6) * final_gain
        return jnp.sum(scaled * reward_head, axis=-1)

    *parts, enters, downs = first_call(native_flag, blocks, gain, enters, downs)
    state = onto(blocks, parts)
    states = []
    for number in range(1, MICRO + STAGES - 1):
        if number < MICRO:
            state = jnp.where(last, entry[number * block : (number + 1) * block], state)
        blocks = sent(state)
        state = onto(blocks, layer_call(blocks, gain, enters, downs))
        if number >= STAGES - 1:
            states.append(state)
    rewards_here = jnp.concatenate([rewarded(state) for state in states])

    mine = jnp.stack([rewards_here, jnp.broadcast_to(kept_sum, (rows_here,))])
    everything = from_everyone(mine, BOTH).reshape(4, 2, 4, 4, 2, rows_here)[3].transpose(1, 2, 0, 3, 4)
    ends = everything[:, :, :, 0]
    rewards = jnp.stack([ends[:, 0, 0], ends[:, 1, 0], ends[:, 1, 1], ends[:, 0, 1]], axis=1).reshape(-1)
    kept_total = jnp.sum(everything[:, :, 0, 1, 0])
    priority = jnp.exp(0.6 * jnp.log(jnp.abs(rewards - returns_all) + 0.05))
    group_best = jnp.max(jnp.where(target_all[:, None] == target_all[None, :], priority[:, None], 0.0), axis=0)
    total = kept_total + jnp.sum(jnp.where(repeat > 0.0, 0.0, group_best))
    part = table_size // STAGES
    own_entries = (row_group * table_size + section * part + jnp.arange(part)).astype(jnp.float32)
    best = jnp.max(jnp.where(target_all[:, None] == own_entries[None, :], priority[:, None], 0.0), axis=0)
    own_old = lax.dynamic_slice_in_dim(old_priority, section * part, part, 0)
    refreshed = jnp.where(best > 0.0, best, own_old)
    weights_out = refreshed * (table_size * 16 / total)
    share = rows_here // STAGES
    rewards_out = lax.dynamic_slice_in_dim(rewards, row_group * rows_here + section * share, share, 0)
    return rewards_out, weights_out


def solution(mesh):
    placed = (
        P("rows", None),
        P("rows"),
        P(),
        P("rows"),
        P("rows", None),
        P("rows"),
        P("section", None),
        P("section", None, "rows"),
        P("section", None, "rows"),
        P("section", "rows", None),
        P(),
        P(),
        P("rows"),
    )
    return jax.shard_map(
        on_device,
        mesh=mesh,
        in_specs=placed,
        out_specs=(P(("rows", "section")), P(("rows", "section"))),
        check_vma=False,
    )
```
